32 devices in a mesh: tiles: 8 (over z, core), feat: 4 (over y, x).
Axes of the slice: x: 2, y: 2, z: 4, core: 2. Of those that a mesh axis runs over, the one named last changes fastest.
Arguments:
- feats: bfloat16 [256, 256, 128], P('tiles', 'feat'), may hold values from -6 to 6
- weight: bfloat16 [128, 128], P('feat'), may hold values from -0.5 to 0.5
- bias: float32 [128], replicated, may hold values from -3 to 3
- neighbours: int32 [256, 16], P('tiles'), may hold values from 0 to 255, as said below
- counts: int32 [256], P('tiles'), may hold values from 4 to 16, as said below
- adj_words: int32 [256, 16, 24, 256], P('tiles', 'feat'), may hold values from 0 to 2047, as said below
- tile_row: int32 [256], replicated, may hold values from 0 to 255, as said below
Outputs:
- new_feats: bfloat16 [256, 256, 128], P('tiles', 'feat')
The draws below stay inside these ranges and needn't reach their ends.
Inputs may be any that keep to these rules, and one draw needn't show every extreme that they name: A permutation of the slide's tiles; slide tile s is stored in the same band as its id, tile_row[s] // 32 == s // 32. Slide ids run row by row over a grid of 8 tile columns. If tile_row[s] == r, every neighbours[r, k] lies within 2 grid rows and 2 grid columns of s (grid row = id // 8, column = id % 8). Slots at or past counts[r] hold valid ids that are not used. `counts`: some tile has all 16 slots live in every draw. `adj_words`: word w holds source cells 11 w to 11 w + 10 in its bits 0 to 10; bits for cells 256 and beyond are zero.
All inputs are finite; a program needn't handle non-finite values.
Results may differ from the reference program's by a relative error of at most 0.0031.
Values may be sent and summed in bfloat16 or wider, within the bound.
No kernel may reach another device: no remote copies, remote signals or barrier semaphores. Data moves between devices by JAX's collectives and lax.ppermute only.
A program may use at most 64 MiB of HBM per device.

```python
import jax
import jax.numpy as jnp
import numpy as np
from jax import lax

CELLS = 256
FEAT = 128
SLOTS = 16
GRID_COLS = 8
TPD = 32
WORDS = 24
NTILES = 256


def band_order(key):
    slide = jnp.arange(NTILES, dtype=jnp.int32)
    noise = jax.random.randint(jax.random.fold_in(key, 3), (NTILES,), 0, 1024)
    score = slide // TPD * (1024 * NTILES) + noise * NTILES + slide
    return jnp.argsort(score, stable=True).astype(jnp.int32)


def draw_tile_row(key, part):
    order = band_order(key)
    return jnp.argsort(order, stable=True).astype(jnp.int32)


def draw_neighbours(key, part):
    order = band_order(key)
    pairs = [(a, b) for a in range(-2, 3) for b in range(-2, 3) if a != 0 or b != 0]
    row_steps = jnp.asarray(np.array([p[0] for p in pairs], dtype=np.int32))
    col_steps = jnp.asarray(np.array([p[1] for p in pairs], dtype=np.int32))
    grid_rows = NTILES // GRID_COLS
    grid_row = order // GRID_COLS
    grid_col = order % GRID_COLS
    score = jax.random.randint(jax.random.fold_in(key, 5), (NTILES, 24), 0, 1024) * 32 + jnp.arange(24, dtype=jnp.int32)[None, :]
    picked = jnp.argsort(score, axis=1, stable=True)[:, :SLOTS]
    near_row = jnp.clip(grid_row[:, None] + row_steps[picked], 0, grid_rows - 1)
    near_col = jnp.clip(grid_col[:, None] + col_steps[picked], 0, GRID_COLS - 1)
    return (near_row * GRID_COLS + near_col).astype(jnp.int32)


def draw_counts(key, part):
    bands = NTILES // TPD
    level = jax.random.randint(jax.random.fold_in(key, 11), (bands,), 0, 4)
    forced = jax.random.randint(jax.random.fold_in(key, 12), (), 0, bands)
    level = jnp.where(jnp.arange(bands, dtype=jnp.int32) == forced, 3, level)
    rows = jnp.arange(NTILES, dtype=jnp.int32)
    tile_level = level[rows // TPD]
    extra = jax.random.randint(jax.random.fold_in(key, 13), (NTILES,), 0, 4 * tile_level + 1)
    total = jnp.minimum(4 + extra, SLOTS)
    spot = forced * TPD + jax.random.randint(jax.random.fold_in(key, 14), (), 0, TPD)
    return jnp.where(rows == spot, SLOTS, total).astype(jnp.int32)


def draw_adj_words(key, part):
    shape = (NTILES, SLOTS, WORDS, CELLS)
    base = jax.random.fold_in(key, 21)
    packed = jax.random.randint(jax.random.fold_in(base, 0), shape, 0, 1 << 11)
    packed = packed & jax.random.randint(jax.random.fold_in(base, 1), shape, 0, 1 << 11)
    packed = packed & jax.random.randint(jax.random.fold_in(base, 2), shape, 0, 1 << 11)
    packed = packed & jax.random.randint(jax.random.fold_in(base, 3), shape, 0, 1 << 11)
    remain = CELLS - 11 * (WORDS - 1)
    limit = jnp.where(jnp.arange(WORDS, dtype=jnp.int32) == WORDS - 1, (1 << remain) - 1, (1 << 11) - 1)
    return (packed & limit[:, None]).astype(jnp.int32)


def levels(stream_key, shape, pieces, least, top_value):
    def one(position, blocks):
        steps = jax.random.uniform(jax.random.fold_in(jax.random.fold_in(stream_key, 6), position), (blocks,), jnp.float32, least / len(pieces), top_value / len(pieces))
        return jnp.repeat(jnp.exp(steps), shape[position] // blocks).reshape((-1,) + (1,) * (len(shape) - position - 1))

    gain = one(*pieces[0])
    for cut in pieces[1:]:
        gain = gain * one(*cut)
    return gain


def normal_values(rng, shape, deviation, reach, pieces=(), kind=jnp.bfloat16):
    values = jax.random.normal(rng, shape, jnp.float32) * deviation
    if len(pieces) > 0:
        values = levels(rng, shape, pieces, -0.22, 0.18) * values
    return jnp.clip(values, min=-reach, max=reach).astype(kind)


def setup_inputs(seed: int = 0) -> dict:
    arg_keys = jax.random.split(jax.random.key(seed), 8)
    feats = normal_values(arg_keys[0], (NTILES, CELLS, FEAT), 1.0, 6.0, ((0, 8), (1, 4)))
    weight = normal_values(arg_keys[1], (FEAT, FEAT), FEAT ** -0.5, 0.5, ((0, 4),))
    bias = normal_values(arg_keys[2], (FEAT,), 0.5, 3.0, (), jnp.float32)
    neighbours = draw_neighbours(jax.random.fold_in(arg_keys[7], 71), 0)
    counts = draw_counts(jax.random.fold_in(arg_keys[7], 71), 0)
    adj_words = draw_adj_words(jax.random.fold_in(arg_keys[7], 71), 0)
    tile_row = draw_tile_row(jax.random.fold_in(arg_keys[7], 71), 0)
    return {"feats": feats, "weight": weight, "bias": bias, "neighbours": neighbours, "counts": counts, "adj_words": adj_words, "tile_row": tile_row}


def unpack_bits(packed):
    shifts = jnp.arange(11, dtype=jnp.int32)
    bit_values = packed[:, :, None, :] >> shifts[None, None, :, None] & 1
    unrolled = bit_values.reshape(packed.shape[0], packed.shape[1] * 11, packed.shape[2])
    return unrolled[:, :CELLS, :].astype(jnp.float32)

def reference(feats, weight, bias, neighbours, counts, adj_words, tile_row):
    source = tile_row[neighbours].astype(jnp.int32)
    live_slots = (jnp.arange(SLOTS, dtype=jnp.int32)[None, :] < counts[:, None]).astype(jnp.float32)

    def one_tile(inputs):
        rows, live_row, packed = inputs
        mask_block = unpack_bits(packed) * live_row[:, None, None]
        gathered = feats[rows].astype(jnp.float32)
        summed = jnp.einsum('kjd,kjf->df', mask_block, gathered)
        degree = lax.optimization_barrier(jnp.sum(mask_block, axis=(0, 1)))
        return (summed, degree)
    summed, degree = lax.map(one_tile, (source, live_slots, adj_words), batch_size=8)
    base = feats.astype(jnp.float32)
    normed = ((summed + base) / jnp.sqrt(degree + 1.0)[:, :, None]).astype(jnp.bfloat16)
    linear = jnp.dot(normed.reshape(-1, FEAT), weight, preferred_element_type=jnp.float32) + bias
    result = base.reshape(-1, FEAT) + jax.nn.relu(linear)
    return result.astype(jnp.bfloat16).reshape(NTILES, CELLS, FEAT)
```

```python
import jax
import jax.numpy as jnp
import numpy as np
from jax import lax
from jax.experimental import pallas as pl
from jax.experimental.pallas import tpu as pltpu
from jax.sharding import PartitionSpec as P

BITS = 11
LANES = 128
SUB = 8
REACH = 16


ANY = pl.BlockSpec(memory_space=pl.ANY)
SMEM = pl.BlockSpec(memory_space=pltpu.SMEM)
VMEM = pl.BlockSpec(memory_space=pltpu.VMEM)


def row_cells(words, cells):
    spare = words * BITS - cells
    assert spare == SUB and words % SUB == 0
    last = BITS - spare
    out = []
    for b in range(BITS):
        for w in range(words if b < BITS - 1 else words - SUB):
            if w < words - 1 or b < last:
                out.append(w * BITS + b)
            else:
                out.append((words - SUB + b - last) * BITS + BITS - 1)
    assert sorted(out) == list(range(cells))
    return np.array(out, dtype=np.int32)


def pack_kernel(group, dst, per_row, last, meta_ref, counts_ref, words_ref, *out_refs):
    chunk_tiles, slots, words, cells = words_ref.shape[1:]
    half = counts_ref.shape[0] // 2
    me, first = meta_ref[0], meta_ref[1]
    lane = lax.broadcasted_iota(jnp.int32, (words, LANES), 1)
    sub = lax.broadcasted_iota(jnp.int32, (SUB, cells), 0)
    for g in range(chunk_tiles // per_row):
        for k in range(slots):
            slot = me * slots + k
            packed = []
            for i in range(per_row):
                tile = g * per_row + i
                low = jnp.where(slot < counts_ref[first + tile], words_ref[0, tile, k], 0)
                high = jnp.where(slot < counts_ref[half + first + tile], words_ref[1, tile, k], 0)
                both = low | (high << 16)
                tail = both[words - SUB :]
                top = ((tail >> (BITS - 1)) & 0x10001) << (sub + last)
                moved = jnp.sum(top, axis=0, keepdims=True)
                kept = tail & ~(0x10001 << (BITS - 1))
                tail = jnp.where(sub == SUB - 1, kept | moved, kept)
                packed.append(jnp.concatenate([both[: words - SUB], tail], axis=0))
            for m in range(group):
                start = (me ^ m) * dst
                block, offset = start // LANES, start % LANES
                row = None
                for i in range(per_row):
                    piece = packed[i][:, :LANES]
                    for h in range(1, cells // LANES):
                        piece = jnp.where(block == h, packed[i][:, h * LANES : (h + 1) * LANES], piece)
                    piece = pltpu.roll(piece, (i * dst + LANES - offset) % LANES, 1)
                    row = piece if row is None else jnp.where(lane >= i * dst, piece, row)
                out_refs[m][g, k] = row


def prepare_kernel(plan, order_ref, perm_ref, *refs):
    pieces, (low_ref, high_ref, held, sem) = refs[: len(plan)], refs[len(plan) :]
    copies = []
    for n, (m, start) in enumerate(plan):
        ref = pieces[n]
        copies.append(pltpu.make_async_copy(ref, held.at[m, pl.ds(start, ref.shape[0])], sem.at[n]))
    for c in copies:
        c.start()
    for c in copies:
        c.wait()
    perm = perm_ref[...]
    half = low_ref.shape[0]

    def put(out_ref, base):
        def step(i, carry):
            row = order_ref[base + i]
            tile = jnp.concatenate([held[m, row] for m in range(held.shape[0])], axis=0)
            out_ref[i] = jnp.dot(perm, tile, preferred_element_type=jnp.float32).astype(jnp.bfloat16)
            return carry

        lax.fori_loop(0, half, step, 0, unroll=4)

    put(low_ref, 0)
    put(high_ref, half)


def main_kernel(group, dst, per_row, chained, meta_ref, src_ref, *refs):
    refs = list(refs)
    words_refs = [refs.pop(0) for _ in range(group)]
    around = [refs.pop(0) for _ in range(4)]
    feats_ref, weight_ref, bias_ref = refs.pop(0), refs.pop(0), refs.pop(0)
    if chained:
        refs.pop(0)
    out_ref, held, sem = refs
    half = around[0].shape[0]
    copies = [
        pltpu.make_async_copy(ref, held.at[pl.ds(n * half, half)], sem.at[n])
        for n, ref in enumerate(around)
    ]
    for c in copies:
        c.start()
    for c in copies:
        c.wait()
    me, first = meta_ref[0], meta_ref[1]
    groups, slots, words = words_refs[0].shape[:3]
    all_slots = group * slots
    weight = weight_ref[...]
    bias = bias_ref[...]

    def rows_of(g, side):
        tile = side * half + first + g * per_row
        sums = [None] * (per_row // 2)
        count = jnp.zeros((words, LANES), jnp.int32)
        for m in range(group):
            for k in range(slots):
                slot = (me ^ m) * slots + k
                packed = words_refs[m][g, k]
                count = count + lax.population_count((packed >> (16 * side)) & 0xFFFF)
                planes = []
                for b in range(BITS):
                    rows = packed if b < BITS - 1 else packed[: words - SUB]
                    planes.append((rows >> (16 * side + b)) & 1)
                mask = jnp.concatenate(planes, axis=0).astype(jnp.float32).astype(jnp.bfloat16).T
                for p in range(per_row // 2):
                    s0 = src_ref[(tile + 2 * p) * all_slots + slot]
                    s1 = src_ref[(tile + 2 * p + 1) * all_slots + slot]
                    pair = jnp.concatenate([held[s0], held[s1]], axis=1)
                    part = mask[2 * p * dst : 2 * (p + 1) * dst]
                    got = jnp.dot(part, pair, preferred_element_type=jnp.float32)
                    sums[p] = got if sums[p] is None else sums[p] + got
        features = feats_ref.shape[3]
        summed = jnp.concatenate(
            [s[j * dst : (j + 1) * dst, j * features : (j + 1) * features] for s in sums for j in range(2)], axis=0
        )
        degree = jnp.sum(count, axis=0, keepdims=True).astype(jnp.float32)
        scale = jnp.sqrt(jnp.broadcast_to(degree, (SUB, LANES)) + 1.0).T[:, :1]
        own = feats_ref[side, pl.ds(g * per_row, per_row)]
        base = own.reshape(per_row * dst, features).astype(jnp.float32)
        normed = ((summed + base) / scale).astype(jnp.bfloat16)
        linear = jnp.dot(normed, weight, preferred_element_type=jnp.float32) + bias
        result = (base + jnp.maximum(linear, 0.0)).astype(jnp.bfloat16)
        out_ref[side, pl.ds(g * per_row, per_row)] = result.reshape(per_row, dst, features)

    for g in range(groups):
        for side in range(2):
            rows_of(g, side)


def swap(x, group, m):
    return lax.ppermute(x, "feat", [(i, i ^ m) for i in range(group)])


def gathered(x, group):
    half = x.shape[0] // 2
    whole = {0: [(0, x)]}
    for m in range(1, group):
        bits = [1 << n for n in range(m.bit_length()) if m >> n & 1]
        if len(bits) == 1:
            whole[m] = [(0, swap(x, group, m))]
        else:
            whole[m] = [
                (start, swap(part[start : start + half] if part.shape[0] > half else part, group, bit))
                for start, bit in ((0, bits[-1]), (half, bits[0]))
                for at, part in whole[m ^ bit]
                if at <= start < at + part.shape[0]
            ]
    return whole


def per_device(feats, weight, bias, neighbours, counts, adj_words, tile_row):
    group, bands = lax.axis_size("feat"), lax.axis_size("tiles")
    me, rank = lax.axis_index("feat"), lax.axis_index("tiles")
    tiles, dst, features = feats.shape
    _, slots, words, cells = adj_words.shape
    half = tiles // 2
    per_row = LANES // dst
    assert half >= REACH and half % per_row == 0 and per_row % 2 == 0 and features == LANES
    rows = half // per_row
    chunks = min(4, rows)
    chunk_rows = rows // chunks
    chunk_tiles = chunk_rows * per_row
    first_tile = rank * tiles

    pieces = gathered(feats, group)
    weight_pieces = [weight] + [swap(weight, group, m) for m in range(1, group)]
    weight_full = jnp.stack(weight_pieces)[jnp.arange(group) ^ me].reshape(-1, features)

    halves = adj_words.reshape(2, half, slots, words, cells)
    exchanged = []
    for c in range(chunks):
        meta = jnp.stack([me, jnp.int32(c * chunk_tiles)])
        shape = jax.ShapeDtypeStruct((chunk_rows, slots, words, LANES), jnp.int32)
        parts = pl.pallas_call(
            lambda *refs: pack_kernel(group, dst, per_row, BITS - (words * BITS - cells), *refs),
            out_shape=[shape] * group,
            grid=(1,),
            in_specs=[
                SMEM,
                SMEM,
                pl.BlockSpec((2, chunk_tiles, slots, words, cells), lambda i, c=c: (0, c, 0, 0, 0)),
            ],
            out_specs=[pl.BlockSpec(shape.shape, lambda i: (0, 0, 0, 0))] * group,
            cost_estimate=pl.CostEstimate(flops=10**9, bytes_accessed=10**6, transcendentals=0),
            name="pack",
        )(meta, counts, halves)
        exchanged.append([parts[0]] + [swap(parts[m], group, m) for m in range(1, group)])

    order = lax.dynamic_slice_in_dim(tile_row, first_tile, tiles, 0) - first_tile
    cell = row_cells(words, cells)
    column = ((cell // dst) ^ me) * dst + cell % dst
    perm = (column[:, None] == jnp.arange(cells, dtype=jnp.int32)[None, :]).astype(jnp.bfloat16)
    plan = [(m, start) for m in range(group) for start, _ in pieces[m]]
    flat = [part for m in range(group) for _, part in pieces[m]]
    side = jax.ShapeDtypeStruct((half, cells, features), jnp.bfloat16)
    low, high = pl.pallas_call(
        lambda *refs: prepare_kernel(plan, *refs),
        out_shape=[side, side],
        in_specs=[SMEM, VMEM] + [ANY] * len(flat),
        out_specs=[VMEM, VMEM],
        scratch_shapes=[
            pltpu.VMEM((group, tiles, dst, features), jnp.bfloat16),
            pltpu.SemaphoreType.DMA((len(flat),)),
        ],
        compiler_params=pltpu.CompilerParams(vmem_limit_bytes=16 * 2**20),
        cost_estimate=pl.CostEstimate(flops=3 * 10**9, bytes_accessed=4 * 10**6, transcendentals=0),
        name="prepare",
    )(order, perm, *flat)
    up = [(i, i + 1) for i in range(bands - 1)]
    before = lax.ppermute(high, "tiles", up)
    after = lax.ppermute(low, "tiles", [(j, i) for i, j in up])

    source = jnp.clip(neighbours - (first_tile - half), 0, 2 * tiles - 1).reshape(-1)
    own = feats.reshape(2, half, dst, features)
    out = None
    for c in range(chunks):
        meta = jnp.stack([me, jnp.int32(c * chunk_tiles)])
        block = pl.BlockSpec((2, chunk_tiles, dst, features), lambda i, c=c: (0, c, 0, 0))
        chained = [] if out is None else [out]
        words_spec = pl.BlockSpec((chunk_rows, slots, words, LANES), lambda i: (0, 0, 0, 0))
        out = pl.pallas_call(
            lambda *refs: main_kernel(group, dst, per_row, c > 0, *refs),
            out_shape=jax.ShapeDtypeStruct(own.shape, own.dtype),
            grid=(1,),
            in_specs=[SMEM, SMEM]
            + [words_spec] * group
            + [ANY] * 4
            + [block, pl.BlockSpec((features, features), lambda i: (0, 0)), pl.BlockSpec((1, features), lambda i: (0, 0))]
            + [ANY] * len(chained),
            out_specs=block,
            scratch_shapes=[
                pltpu.VMEM((4 * half, cells, features), jnp.bfloat16),
                pltpu.SemaphoreType.DMA((4,)),
            ],
            input_output_aliases={9 + group: 0} if chained else {},
            compiler_params=pltpu.CompilerParams(vmem_limit_bytes=24 * 2**20),
            cost_estimate=pl.CostEstimate(flops=3 * 10**9, bytes_accessed=5 * 10**6, transcendentals=0),
            name="main",
        )(meta, source, *exchanged[c], before, low, high, after, own, weight_full, bias[None, :], *chained)
    return out.reshape(feats.shape)


def solution(mesh):
    return jax.shard_map(
        per_device,
        mesh=mesh,
        in_specs=(
            P("tiles", "feat", None),
            P("feat", None),
            P(),
            P("tiles", None),
            P("tiles"),
            P("tiles", "feat", None, None),
            P(),
        ),
        out_specs=P("tiles", "feat", None),
        check_vma=False,
    )
```

```python
import functools

import jax
import jax.numpy as jnp
import numpy as np
from jax import lax
from jax.experimental import pallas as pl
from jax.experimental.pallas import tpu as pltpu
from jax.sharding import PartitionSpec as P

BITS = 11
LANES = 128
SUB = 8
REACH = 16


HBM = pl.BlockSpec(memory_space=pltpu.HBM)
SMEM = pl.BlockSpec(memory_space=pltpu.SMEM)
VMEM = pl.BlockSpec(memory_space=pltpu.VMEM)


def row_cells(words, cells):
    spare = words * BITS - cells
    assert spare == SUB and words % SUB == 0
    last, tail = BITS - spare, words - SUB
    order = [(b, w) for b in range(BITS) for w in range(tail)]
    order += [(b, w) for b in range(BITS - 1) for w in range(tail, words)]
    out = []
    for b, w in order:
        moved = w == words - 1 and b >= last
        out.append((tail + b - last) * BITS + BITS - 1 if moved else w * BITS + b)
    assert sorted(out) == list(range(cells))
    return np.array(out, dtype=np.int32)


def pack_kernel(group, dst, per_row, last, sizes, counts_ref, words_ref, *out_refs):
    me = lax.axis_index("feat")
    tiles, slots, words, cells = words_ref.shape
    rows = tiles // per_row
    lane = lax.broadcasted_iota(jnp.int32, (words, LANES), 1)
    sub = lax.broadcasted_iota(jnp.int32, (SUB, cells), 0)

    def row_of(rank, at, c, g, carry):
        for k in range(slots):
            packed = []
            for i in range(per_row):
                tile = g * per_row + i
                live = rank * slots + k < counts_ref[pl.program_id(0) * tiles + tile]
                both = jnp.where(live, words_ref[tile, k], 0)
                tail = both[words - SUB :]
                top = ((tail >> (BITS - 1)) & 1) << (sub + last)
                moved = jnp.sum(top, axis=0, keepdims=True)
                kept = tail & ((1 << (BITS - 1)) - 1)
                tail = jnp.where(sub == SUB - 1, kept | moved, kept)
                packed.append(jnp.concatenate([both[: words - SUB], tail], axis=0))
            for m in range(group):
                start = (rank ^ m) * dst
                block, offset = start // LANES, start % LANES
                row = None
                for i in range(per_row):
                    piece = packed[i][:, block * LANES : (block + 1) * LANES]
                    shift = (i * dst + LANES - offset) % LANES
                    if shift:
                        piece = pltpu.roll(piece, shift, 1)
                    row = piece if row is None else jnp.where(lane >= i * dst, piece, row)
                out_refs[c * group + m][at + g, k] = row.astype(jnp.int16)
        return carry

    for rank in range(group):
        at = 0
        for c, size in enumerate(sizes):
            first, step = at // rows, pl.program_id(0)

            @pl.when((me == rank) & (step >= first) & (step < first + size // rows))
            def _(rank=rank, c=c, first=first):
                lax.fori_loop(0, rows, functools.partial(row_of, rank, (step - first) * rows, c), 0, unroll=min(rows, 4))

            at += size


def prepare_kernel(plan, order_ref, perm_ref, *refs):
    pieces, (low_ref, high_ref, held, sem) = refs[: len(plan)], refs[len(plan) :]
    copies = []
    for n, (m, start) in enumerate(plan):
        ref = pieces[n]
        copies.append(pltpu.make_async_copy(ref, held.at[m, pl.ds(start, ref.shape[0])], sem.at[n]))
    for c in copies:
        c.start()
    for c in copies:
        c.wait()
    perm = perm_ref[...]
    half = low_ref.shape[0]

    def put(out_ref, base):
        def step(i, carry):
            tiles = []
            for j in range(2):
                row = order_ref[base + 2 * i + j]
                tiles.append(jnp.concatenate([held[m, row] for m in range(held.shape[0])], axis=0))
            got = jnp.dot(perm, jnp.concatenate(tiles, axis=1), preferred_element_type=jnp.float32)
            for j in range(2):
                out_ref[2 * i + j] = got[:, j * LANES : (j + 1) * LANES].astype(jnp.bfloat16)
            return carry

        lax.fori_loop(0, half // 2, step, 0, unroll=4)

    put(low_ref, 0)
    put(high_ref, half)


def main_kernel(group, dst, per_row, *refs):
    rows = refs[-1].shape[0] - 1
    batch = min(4, rows // 2)
    sets = [[[pltpu.ACC(q)((2 * dst, 2 * LANES), jnp.float32) for _ in range(per_row // 2)] for _ in range(2)] for q in range(2)]
    linear = [pltpu.ACC(q)((batch * LANES, 2 * LANES), jnp.float32) for q in range(2)]
    pl.run_scoped(lambda a, b: main_body(group, dst, per_row, batch, a, b, *refs), sets, linear)


def main_body(group, dst, per_row, batch, accs, products, src_ref, *refs):
    *ins, weight_ref, bias_ref, out_ref, held, words_all, feats_all, sem, sums_ref, degrees_ref = refs
    half = ins[0].shape[0]
    copies = [(ref, held.at[pl.ds(n * half, half)]) for n, ref in enumerate(ins[:4])]
    copies.append((ins[4], feats_all))
    starts = [0] * group
    for n, ref in enumerate(ins[5:]):
        m = n % group
        copies.append((ref, words_all.at[m, pl.ds(starts[m], ref.shape[0])]))
        starts[m] += ref.shape[0]
    copies = [pltpu.make_async_copy(a, b, sem.at[n]) for n, (a, b) in enumerate(copies)]
    for c in copies:
        c.start()
    for a in [a for by_mxu in accs for by_set in by_mxu for a in by_set] + products:
        pltpu.matmul_pop(a)
    for c in copies:
        c.wait()
    me = lax.axis_index("feat")
    rows, slots, words = words_all.shape[1:4]
    all_slots = group * slots
    bias = bias_ref[...]
    features = bias.shape[1]
    pairs = per_row // 2
    one, zero = jnp.bfloat16(1), jnp.bfloat16(0)
    upper = lax.broadcasted_iota(jnp.int32, (2 * SUB, LANES), 0) >= SUB
    bits = [jnp.where(upper, 2 << b, 1 << b).astype(jnp.int16) for b in range(0, BITS - 1, 2)]

    def finished(which):
        got = [pltpu.matmul_pop(accs[0][which][p]) + pltpu.matmul_pop(accs[1][which][p]) for p in range(pairs)]
        return jnp.concatenate(
            [s[j * dst : (j + 1) * dst, j * features : (j + 1) * features] for s in got for j in range(2)], axis=0
        )

    def row_of(row, which):
        tile = row * per_row
        count = jnp.zeros((SUB, LANES), jnp.int32)
        turn = 0
        for m in range(group):
            for k in range(slots):
                slot = (me ^ m) * slots + k
                parts = [words_all[m, row, k, w : w + SUB] for w in range(0, words, SUB)]
                for part in parts:
                    count = count + lax.population_count(part.astype(jnp.int32))
                front = jnp.concatenate(parts[:-1], axis=0)
                back = jnp.concatenate([parts[-1]] * 2, axis=0)
                planes = [jnp.where((front & jnp.int16(1 << b)) != 0, one, zero) for b in range(BITS)]
                planes += [jnp.where((back & bit) != 0, one, zero) for bit in bits]
                mask = jnp.concatenate(planes, axis=0).T
                mxu = turn % 2
                for p in range(pairs):
                    s0 = src_ref[(tile + 2 * p) * all_slots + slot]
                    s1 = src_ref[(tile + 2 * p + 1) * all_slots + slot]
                    register = (turn // 2 * pairs + p) % 2
                    pltpu.matmul_push_rhs(jnp.concatenate([held[s0], held[s1]], axis=1), register, mxu)
                    part = mask[2 * p * dst : 2 * (p + 1) * dst]
                    pltpu.matmul_acc_lhs(accs[mxu][which][p], part, load_staged_rhs=register)
                turn += 1
                if turn == 6:
                    sums_ref[row] = finished(1 - which)
        degrees_ref[row] = jnp.broadcast_to(jnp.sum(count, axis=0, keepdims=True), (SUB, LANES)).astype(jnp.float32)

    def step(n, carry):
        for j in range(2):
            row_of(2 * n + j, j)
        return carry

    lax.fori_loop(0, rows // 2, step, 0)
    sums_ref[rows] = finished(1)

    for q in range(2):
        pltpu.matmul_push_rhs(weight_ref[...], 0, q)
    for n in range(0, rows, batch):
        q = n // batch % 2
        bases, wide = [], []
        for row in range(n, n + batch):
            scale = jnp.sqrt(degrees_ref[row] + 1.0).T[:, :1]
            base = feats_all[row * per_row : (row + 1) * per_row].reshape(LANES, features).astype(jnp.float32)
            normed = ((sums_ref[row + 1] + base) / scale).astype(jnp.bfloat16)
            bases.append(base)
            wide.append(jnp.concatenate([normed, jnp.zeros_like(normed)], axis=1))
        pltpu.matmul_acc_lhs(products[q], jnp.concatenate(wide, axis=0), load_staged_rhs=0 if n // batch < 2 else None)
        linear = pltpu.matmul_pop(products[q])[:, :features] + bias
        result = (jnp.concatenate(bases, axis=0) + jnp.maximum(linear, 0.0)).astype(jnp.bfloat16)
        out_ref[n * per_row : (n + batch) * per_row] = result.reshape(batch * per_row, dst, features)


def swap(x, group, m):
    return lax.ppermute(x, "feat", [(i, i ^ m) for i in range(group)])


def gathered(x, group):
    half = x.shape[0] // 2
    direct = [1 << n for n in range(group.bit_length() - 1)]
    whole = {0: [(0, x)]} | {m: [(0, swap(x, group, m))] for m in direct}
    for m in range(1, group):
        bits = [bit for bit in direct if m & bit]
        if len(bits) > 1:
            whole[m] = [
                (start, swap(part[start : start + half] if part.shape[0] > half else part, group, bit))
                for start, bit in ((0, bits[-1]), (half, bits[0]))
                for at, part in whole[m ^ bit]
                if at <= start < at + part.shape[0]
            ]
    return whole


def per_device(feats, weight, bias, neighbours, counts, adj_words, tile_row):
    group, bands = lax.axis_size("feat"), lax.axis_size("tiles")
    me, rank = lax.axis_index("feat"), lax.axis_index("tiles")
    tiles, dst, features = feats.shape
    _, slots, words, cells = adj_words.shape
    half = tiles // 2
    per_row = LANES // dst
    assert half >= REACH and tiles % per_row == 0 and per_row % 2 == 0 and features == LANES
    rows = tiles // per_row
    sizes = [rows // 4, rows - rows // 4]
    first_tile = rank * tiles

    shapes = [jax.ShapeDtypeStruct((n, slots, words, LANES), jnp.int16) for n in sizes for _ in range(group)]
    block = min(sizes) * per_row
    packed = pl.pallas_call(
        lambda *refs: pack_kernel(group, dst, per_row, BITS - (words * BITS - cells), sizes, *refs),
        out_shape=shapes,
        grid=(tiles // block,),
        in_specs=[SMEM, pl.BlockSpec((block, slots, words, cells), lambda i: (i, 0, 0, 0))],
        out_specs=[pl.BlockSpec(s.shape, lambda i: (0, 0, 0, 0)) for s in shapes],
        cost_estimate=pl.CostEstimate(flops=3 * 10**9, bytes_accessed=5 * 10**6, transcendentals=0),
        name="pack",
    )(counts, adj_words)

    pieces = gathered(feats, group)
    exchanged = []
    for c in range(len(sizes)):
        parts = packed[c * group : (c + 1) * group]
        exchanged += [parts[0]] + [swap(parts[m], group, m) for m in range(1, group)]
    weight_pieces = [weight] + [swap(weight, group, m) for m in range(1, group)]
    weight_full = jnp.stack(weight_pieces)[jnp.arange(group) ^ me].reshape(-1, features)
    weight_wide = jnp.pad(weight_full, ((0, LANES), (0, LANES)))

    order = lax.dynamic_slice_in_dim(tile_row, first_tile, tiles, 0) - first_tile
    cell = row_cells(words, cells)
    column = ((cell // dst) ^ me) * dst + cell % dst
    perm = (column[:, None] == jnp.arange(cells, dtype=jnp.int32)[None, :]).astype(jnp.bfloat16)
    plan = [(m, start) for m in range(group) for start, _ in pieces[m]]
    flat = [part for m in range(group) for _, part in pieces[m]]
    side = jax.ShapeDtypeStruct((half, cells, features), jnp.bfloat16)
    low, high = pl.pallas_call(
        lambda *refs: prepare_kernel(plan, *refs),
        out_shape=[side, side],
        in_specs=[SMEM, VMEM] + [HBM] * len(flat),
        out_specs=[VMEM, VMEM],
        scratch_shapes=[
            pltpu.VMEM((group, tiles, dst, features), jnp.bfloat16),
            pltpu.SemaphoreType.DMA((len(flat),)),
        ],
        cost_estimate=pl.CostEstimate(flops=3 * 10**9, bytes_accessed=4 * 10**6, transcendentals=0),
        name="prepare",
    )(order, perm, *flat)
    up = [(i, i + 1) for i in range(bands - 1)]
    before = lax.ppermute(high, "tiles", up)
    after = lax.ppermute(low, "tiles", [(j, i) for i, j in up])

    source = jnp.clip(neighbours - (first_tile - half), 0, 2 * tiles - 1).reshape(-1)
    return pl.pallas_call(
        lambda *refs: main_kernel(group, dst, per_row, *refs),
        out_shape=jax.ShapeDtypeStruct(feats.shape, feats.dtype),
        in_specs=[SMEM] + [HBM] * (5 + len(exchanged)) + [VMEM] * 2,
        out_specs=VMEM,
        scratch_shapes=[
            pltpu.VMEM((4 * half, cells, features), jnp.bfloat16),
            pltpu.VMEM((group, rows, slots, words, LANES), jnp.int16),
            pltpu.VMEM(feats.shape, jnp.bfloat16),
            pltpu.SemaphoreType.DMA((5 + len(exchanged),)),
            pltpu.VMEM((rows + 1, LANES, features), jnp.float32),
            pltpu.VMEM((rows + 1, SUB, LANES), jnp.float32),
        ],
        cost_estimate=pl.CostEstimate(flops=10**10, bytes_accessed=10**7, transcendentals=0),
        name="main",
    )(source, before, low, high, after, feats, *exchanged, weight_wide, bias[None, :])


def solution(mesh):
    return jax.shard_map(
        per_device,
        mesh=mesh,
        in_specs=(
            P("tiles", "feat", None),
            P("feat", None),
            P(),
            P("tiles", None),
            P("tiles"),
            P("tiles", "feat", None, None),
            P(),
        ),
        out_specs=P("tiles", "feat", None),
        check_vma=False,
    )
```

```python
import functools

import jax
import jax.numpy as jnp
import numpy as np
from jax import lax
from jax.experimental import pallas as pl
from jax.experimental.pallas import tpu as pltpu
from jax.sharding import PartitionSpec as P

BITS = 11
LANES = 128
SUB = 8
REACH = 16


HBM = pl.BlockSpec(memory_space=pltpu.HBM)
SMEM = pl.BlockSpec(memory_space=pltpu.SMEM)
VMEM = pl.BlockSpec(memory_space=pltpu.VMEM)


def row_cells(words, cells):
    spare = words * BITS - cells
    assert spare == SUB and words % SUB == 0
    last, tail = BITS - spare, words - SUB
    order = [(b, w) for b in range(BITS) for w in range(tail)]
    order += [(b, w) for b in range(BITS - 1) for w in range(tail, words)]
    out = []
    for b, w in order:
        moved = w == words - 1 and b >= last
        out.append((tail + b - last) * BITS + BITS - 1 if moved else w * BITS + b)
    assert sorted(out) == list(range(cells))
    return np.array(out, dtype=np.int32)


def pack_kernel(group, dst, per_row, last, sizes, counts_ref, words_ref, *out_refs):
    me = lax.axis_index("feat")
    tiles, slots, words, cells = words_ref.shape
    rows = tiles // per_row
    lane = lax.broadcasted_iota(jnp.int32, (words, LANES), 1)
    sub = lax.broadcasted_iota(jnp.int32, (SUB, cells), 0)

    def row_of(rank, at, c, g, carry):
        for k in range(slots):
            packed = []
            for i in range(per_row):
                tile = g * per_row + i
                live = rank * slots + k < counts_ref[pl.program_id(0) * tiles + tile]
                both = jnp.where(live, words_ref[tile, k], 0)
                tail = both[words - SUB :]
                top = ((tail >> (BITS - 1)) & 1) << (sub + last)
                moved = jnp.sum(top, axis=0, keepdims=True)
                kept = tail & ((1 << (BITS - 1)) - 1)
                tail = jnp.where(sub == SUB - 1, kept | moved, kept)
                packed.append(jnp.concatenate([both[: words - SUB], tail], axis=0))
            for m in range(group):
                start = (rank ^ m) * dst
                block, offset = start // LANES, start % LANES
                row = None
                for i in range(per_row):
                    piece = packed[i][:, block * LANES : (block + 1) * LANES]
                    shift = (i * dst + LANES - offset) % LANES
                    if shift:
                        piece = pltpu.roll(piece, shift, 1)
                    row = piece if row is None else jnp.where(lane >= i * dst, piece, row)
                out_refs[c * group + m][at + g, k] = row.astype(jnp.int16)
        return carry

    for rank in range(group):
        at = 0
        for c, size in enumerate(sizes):
            first, step = at // rows, pl.program_id(0)

            @pl.when((me == rank) & (step >= first) & (step < first + size // rows))
            def _(rank=rank, c=c, first=first):
                lax.fori_loop(0, rows, functools.partial(row_of, rank, (step - first) * rows, c), 0, unroll=max(1, min(rows, 16 // group)))

            at += size


def arrange_kernel(near, inner_bits, outer_bits, tiles_ref, *refs):
    pieces, outs = refs[:near], list(refs[near:])
    tiles = pieces[0].shape[0]
    half = tiles // 2
    first = lax.axis_index("tiles") * tiles
    odd = lax.axis_index("tiles") % 2
    for side, bits in ((1 - odd, inner_bits), (odd, outer_bits)):
        together = outs.pop(0)
        alone = {n: outs.pop(0) for n in bits}
        for i in range(half):
            row = tiles_ref[first + side * half + i] - first
            for n in range(near):
                tile = pieces[n][row]
                together[n, i] = tile
                if n in alone:
                    alone[n][i] = tile


def assemble_kernel(group, places, perm_ref, *refs):
    perm = perm_ref[...]
    odd = lax.axis_index("tiles") % 2
    near = [0] + [1 << n for n in range(group.bit_length() - 1)]
    far = [m for m in range(group) if m not in near]
    per_side = 1 + len(far)
    tiles_ref = refs[2 * per_side + group] if len(refs) > 2 * per_side + group else refs[-1]

    def step(base, side, i, carry):
        pair = []
        for j in range(2):
            tile = 2 * i + j
            cut = {m: side[0][n, tile] for n, m in enumerate(near)} | {m: side[1 + n][tile] for n, m in enumerate(far)}
            pair.append(jnp.concatenate([cut[m] for m in range(group)], axis=0))
        got = jnp.dot(perm, jnp.concatenate(pair, axis=1), preferred_element_type=jnp.float32)
        for j in range(2):
            tiles_ref[base + 2 * i + j] = got[:, j * LANES : (j + 1) * LANES].astype(jnp.bfloat16)
        return carry

    for n, (even_place, odd_place) in enumerate(places):
        side = refs[n * per_side : (n + 1) * per_side]
        half = side[0].shape[1]
        base = jnp.where(odd == 1, odd_place * half, even_place * half)
        lax.fori_loop(0, half // 2, functools.partial(step, base, side), 0, unroll=4)
    if tiles_ref is not refs[-1]:
        weights, weight_ref = refs[2 * per_side : 2 * per_side + group], refs[-1]
        me = lax.axis_index("feat")
        _, features = weights[0].shape
        rows = []
        for rank in range(group):
            row = weights[0][...].astype(jnp.float32)
            for m in range(1, group):
                row = jnp.where(me ^ m == rank, weights[m][...].astype(jnp.float32), row)
            rows.append(row)
        weight_ref[...] = jnp.zeros_like(weight_ref)
        weight_ref[:features, :features] = jnp.concatenate(rows, axis=0).astype(jnp.bfloat16)


def main_kernel(group, dst, per_row, *refs):
    rows = refs[-1].shape[0] - 1
    batch = min(4, rows // 2)
    sets = [[[pltpu.ACC(q)((2 * dst, 2 * LANES), jnp.float32) for _ in range(per_row // 2)] for _ in range(2)] for q in range(2)]
    linear = [pltpu.ACC(q)((batch * LANES, 2 * LANES), jnp.float32) for q in range(2)]
    pl.run_scoped(lambda a, b: main_body(group, dst, per_row, batch, a, b, *refs), sets, linear)


def main_body(group, dst, per_row, batch, accs, products, neighbours_ref, *refs):
    held, weight_ref, bias_ref, feats_ref, *ins, out_ref, sums_ref, degrees_ref = refs
    chunk_refs = [ins[n : n + group] for n in range(0, len(ins), group)]
    for a in [a for by_mxu in accs for by_set in by_mxu for a in by_set] + products:
        pltpu.matmul_pop(a)
    me = lax.axis_index("feat")
    rows = sums_ref.shape[0] - 1
    slots, words = ins[0].shape[1:3]
    tiles, half = neighbours_ref.shape[1], held.shape[0] // 4
    origin = lax.axis_index("tiles") * tiles - half
    bias = bias_ref[...]
    features = bias.shape[1]
    pairs = per_row // 2
    one, zero = jnp.bfloat16(1), jnp.bfloat16(0)
    upper = lax.broadcasted_iota(jnp.int32, (2 * SUB, LANES), 0) >= SUB
    bits = [jnp.where(upper, 2 << b, 1 << b).astype(jnp.int16) for b in range(0, BITS - 1, 2)]

    def source(slot, tile):
        return jnp.clip(neighbours_ref[slot, tile] - origin, 0, 4 * half - 1)

    def finished(which):
        got = [pltpu.matmul_pop(accs[0][which][p]) + pltpu.matmul_pop(accs[1][which][p]) for p in range(pairs)]
        return jnp.concatenate(
            [s[j * dst : (j + 1) * dst, j * features : (j + 1) * features] for s in got for j in range(2)], axis=0
        )

    def row_of(words_refs, first, row, which):
        tile = row * per_row
        count = jnp.zeros((SUB, LANES), jnp.int32)
        turn = 0
        for m in range(group):
            for k in range(slots):
                slot = (me ^ m) * slots + k
                parts = [words_refs[m][row - first, k, w : w + SUB] for w in range(0, words, SUB)]
                for part in parts:
                    count = count + lax.population_count(part.astype(jnp.int32))
                front = jnp.concatenate(parts[:-1], axis=0)
                back = jnp.concatenate([parts[-1]] * 2, axis=0)
                planes = [jnp.where((front & jnp.int16(1 << b)) != 0, one, zero) for b in range(BITS)]
                planes += [jnp.where((back & bit) != 0, one, zero) for bit in bits]
                mask = jnp.concatenate(planes, axis=0).T
                mxu = turn % 2
                for p in range(pairs):
                    s0, s1 = (source(slot, tile + 2 * p + j) for j in range(2))
                    register = (turn // 2 * pairs + p) % 2
                    pltpu.matmul_push_rhs(jnp.concatenate([held[s0], held[s1]], axis=1), register, mxu)
                    part = mask[2 * p * dst : 2 * (p + 1) * dst]
                    pltpu.matmul_acc_lhs(accs[mxu][which][p], part, load_staged_rhs=register)
                turn += 1
                if turn == 6:
                    sums_ref[row] = finished(1 - which)
        degrees_ref[row] = jnp.broadcast_to(jnp.sum(count, axis=0, keepdims=True), (SUB, LANES)).astype(jnp.float32)

    first = 0
    for words_refs in chunk_refs:
        size = words_refs[0].shape[0]

        def step(n, carry, words_refs=words_refs, first=first):
            for j in range(2):
                row_of(words_refs, first, first + 2 * n + j, j)
            return carry

        lax.fori_loop(0, size // 2, step, 0)
        first += size
    sums_ref[rows] = finished(1)

    for q in range(2):
        pltpu.matmul_push_rhs(weight_ref[...], 0, q)
    for n in range(0, rows, batch):
        q = n // batch % 2
        bases, wide = [], []
        for row in range(n, n + batch):
            scale = jnp.sqrt(degrees_ref[row] + 1.0).T[:, :1]
            base = feats_ref[row * per_row : (row + 1) * per_row].reshape(LANES, features).astype(jnp.float32)
            normed = ((sums_ref[row + 1] + base) / scale).astype(jnp.bfloat16)
            bases.append(base)
            wide.append(jnp.concatenate([normed, jnp.zeros_like(normed)], axis=1))
        pltpu.matmul_acc_lhs(products[q], jnp.concatenate(wide, axis=0), load_staged_rhs=0 if n // batch < 2 else None)
        linear = pltpu.matmul_pop(products[q])[:, :features] + bias
        result = (jnp.concatenate(bases, axis=0) + jnp.maximum(linear, 0.0)).astype(jnp.bfloat16)
        out_ref[n * per_row : (n + batch) * per_row] = result.reshape(batch * per_row, dst, features)


def swap(x, group, m):
    return lax.ppermute(x, "feat", [(i, i ^ m) for i in range(group)])


def per_device(feats, weight, bias, neighbours, counts, adj_words, tile_row):
    group, bands = lax.axis_size("feat"), lax.axis_size("tiles")
    me = lax.axis_index("feat")
    tiles, dst, features = feats.shape
    _, slots, words, cells = adj_words.shape
    half = tiles // 2
    per_row = LANES // dst
    rows = tiles // per_row
    assert half >= REACH and rows % 4 == 0 and per_row % 2 == 0 and bands % 2 == 0 and features == LANES
    sizes = [rows // 2, rows - rows // 2]

    shapes = [jax.ShapeDtypeStruct((n, slots, words, LANES), jnp.int16) for n in sizes for _ in range(group)]
    block = min(sizes) * per_row
    packed = pl.pallas_call(
        lambda *refs: pack_kernel(group, dst, per_row, BITS - (words * BITS - cells), sizes, *refs),
        out_shape=shapes,
        grid=(tiles // block,),
        in_specs=[SMEM, pl.BlockSpec((block, slots, words, cells), lambda i: (i, 0, 0, 0))],
        out_specs=[pl.BlockSpec(s.shape, lambda i: (0, 0, 0, 0)) for s in shapes],
        cost_estimate=pl.CostEstimate(flops=3 * 10**9, bytes_accessed=5 * 10**6, transcendentals=0),
        name="pack",
    )(counts, adj_words)

    direct = [1 << n for n in range(group.bit_length() - 1)]
    far = [m for m in range(group) if m & (m - 1)]
    near = [feats] + [swap(feats, group, m) for m in direct]
    weight_pieces = [weight] + [swap(weight, group, m) for m in range(1, group)]
    inner_bits = list(range(1, len(direct)))
    outer_bits = list(range(2, len(direct) + 1))
    together = jax.ShapeDtypeStruct((len(near), half, dst, features), jnp.bfloat16)
    alone = jax.ShapeDtypeStruct((half, dst, features), jnp.bfloat16)
    inner, *rest = pl.pallas_call(
        lambda *refs: arrange_kernel(len(near), inner_bits, outer_bits, *refs),
        out_shape=[together] + [alone] * len(inner_bits) + [together] + [alone] * len(outer_bits),
        in_specs=[SMEM] + [VMEM] * len(near),
        out_specs=[VMEM] * (2 + len(inner_bits) + len(outer_bits)),
        compiler_params=pltpu.CompilerParams(vmem_limit_bytes=4 * 2**20),
        cost_estimate=pl.CostEstimate(flops=10**9, bytes_accessed=10**6, transcendentals=0),
        name="arrange",
    )(tile_row, *near)
    inners = {direct[n - 1]: part for n, part in zip(inner_bits, rest)}
    outer, *rest = rest[len(inner_bits) :]
    outers = {direct[n - 1]: part for n, part in zip(outer_bits, rest)}
    for m in far:
        bits = [bit for bit in direct if m & bit]
        inners[m] = swap(inners[m ^ bits[-1]], group, bits[-1])
        outers[m] = swap(outers[m ^ bits[0]], group, bits[0])
    inners, outers = [inner] + [inners[m] for m in far], [outer] + [outers[m] for m in far]
    exchanged = []
    for c in range(len(sizes)):
        parts = packed[c * group : (c + 1) * group]
        exchanged += [parts[0]] + [swap(parts[m], group, m) for m in range(1, group)]

    inside = [(i, i ^ 1) for i in range(bands)]
    across = [pair for i in range(1, bands - 1, 2) for pair in ((i, i + 1), (i + 1, i))]
    from_inside, from_across = [], []
    for n in range(len(inners)):
        from_across.append(lax.ppermute(outers[n], "tiles", across))
        from_inside.append(lax.ppermute(inners[n], "tiles", inside))

    cell = row_cells(words, cells)
    column = ((cell // dst) ^ me) * dst + cell % dst
    perm = (column[:, None] == jnp.arange(cells, dtype=jnp.int32)[None, :]).astype(jnp.bfloat16)
    reachable_shape = jax.ShapeDtypeStruct((4 * half, cells, features), jnp.bfloat16)
    assemble = functools.partial(
        pl.pallas_call,
        compiler_params=pltpu.CompilerParams(vmem_limit_bytes=4 * 2**20),
        cost_estimate=pl.CostEstimate(flops=2 * 10**9, bytes_accessed=4 * 10**6, transcendentals=0),
        name="assemble",
    )
    sides = inners + outers + weight_pieces
    reachable, weight_wide = assemble(
        lambda *refs: assemble_kernel(group, ((2, 1), (1, 2)), *refs),
        out_shape=[reachable_shape, jax.ShapeDtypeStruct((2 * features, 2 * features), jnp.bfloat16)],
        in_specs=[VMEM] * (1 + len(sides)),
        out_specs=[VMEM] * 2,
    )(perm, *sides)
    sides = from_inside + from_across
    reachable = assemble(
        lambda *refs: assemble_kernel(group, ((3, 0), (0, 3)), *refs),
        out_shape=reachable_shape,
        in_specs=[VMEM] * (2 + len(sides)),
        out_specs=VMEM,
        input_output_aliases={1 + len(sides): 0},
    )(perm, *sides, reachable)

    return pl.pallas_call(
        lambda *refs: main_kernel(group, dst, per_row, *refs),
        out_shape=jax.ShapeDtypeStruct(feats.shape, feats.dtype),
        in_specs=[SMEM] + [VMEM] * (4 + len(exchanged)),
        out_specs=VMEM,
        scratch_shapes=[
            pltpu.VMEM((rows + 1, LANES, features), jnp.float32),
            pltpu.VMEM((rows + 1, SUB, LANES), jnp.float32),
        ],
        compiler_params=pltpu.CompilerParams(vmem_limit_bytes=12 * 2**20),
        cost_estimate=pl.CostEstimate(flops=10**10, bytes_accessed=10**7, transcendentals=0),
        name="main",
    )(neighbours.T, reachable, weight_wide, bias[None, :], feats, *exchanged)


def solution(mesh):
    return jax.shard_map(
        per_device,
        mesh=mesh,
        in_specs=(
            P("tiles", "feat", None),
            P("feat", None),
            P(),
            P("tiles", None),
            P("tiles"),
            P("tiles", "feat", None, None),
            P(),
        ),
        out_specs=P("tiles", "feat", None),
        check_vma=False,
    )
```

```python
import functools
import math

import jax
import jax.numpy as jnp
import numpy as np
from jax import lax
from jax.experimental import pallas as pl
from jax.experimental.pallas import tpu as pltpu
from jax.sharding import PartitionSpec as P

BITS = 11
LANES = 128
SUB = 8
REACH = 16


HBM = pl.BlockSpec(memory_space=pltpu.HBM)
SMEM = pl.BlockSpec(memory_space=pltpu.SMEM)
VMEM = pl.BlockSpec(memory_space=pltpu.VMEM)


def row_cells(words, cells):
    spare = words * BITS - cells
    assert spare == SUB and words % SUB == 0
    last, tail = BITS - spare, words - SUB
    order = [(b, w) for b in range(BITS) for w in range(tail)]
    order += [(b, w) for b in range(BITS - 1) for w in range(tail, words)]
    out = []
    for b, w in order:
        moved = w == words - 1 and b >= last
        out.append((tail + b - last) * BITS + BITS - 1 if moved else w * BITS + b)
    assert sorted(out) == list(range(cells))
    return np.array(out, dtype=np.int32)


def pack_kernel(group, dst, per_row, last, sizes, counts_ref, words_ref, *out_refs):
    me = lax.axis_index("feat")
    tiles, slots, words, cells = words_ref.shape
    rows = tiles // per_row
    lane = lax.broadcasted_iota(jnp.int32, (words, LANES), 1)
    sub = lax.broadcasted_iota(jnp.int32, (SUB, cells), 0)

    def row_of(rank, at, c, g, carry):
        for k in range(slots):
            packed = []
            for i in range(per_row):
                tile = g * per_row + i
                live = rank * slots + k < counts_ref[pl.program_id(0) * tiles + tile]
                both = jnp.where(live, words_ref[tile, k], 0)
                tail = both[words - SUB :]
                top = ((tail >> (BITS - 1)) & 1) << (sub + last)
                moved = jnp.sum(top, axis=0, keepdims=True)
                kept = tail & ((1 << (BITS - 1)) - 1)
                tail = jnp.where(sub == SUB - 1, kept | moved, kept)
                packed.append(jnp.concatenate([both[: words - SUB], tail], axis=0))
            for m in range(group):
                start = (rank ^ m) * dst
                block, offset = start // LANES, start % LANES
                row = None
                for i in range(per_row):
                    piece = packed[i][:, block * LANES : (block + 1) * LANES]
                    shift = (i * dst + LANES - offset) % LANES
                    if shift:
                        piece = pltpu.roll(piece, shift, 1)
                    row = piece if row is None else jnp.where(lane >= i * dst, piece, row)
                out_refs[c * group + m][at + g, k] = row.astype(jnp.int16)
        return carry

    for rank in range(group):
        at = 0
        for c, size in enumerate(sizes):
            first, step = at // rows, pl.program_id(0)

            @pl.when((me == rank) & (step >= first) & (step < first + size // rows))
            def _(rank=rank, c=c, first=first):
                lax.fori_loop(0, rows, functools.partial(row_of, rank, (step - first) * rows, c), 0, unroll=max(1, min(rows, 16 // group)))

            at += size


def arrange_kernel(near, inner_bits, outer_bits, tiles_ref, *refs):
    pieces, outs = refs[:near], list(refs[near:])
    tiles = pieces[0].shape[0]
    half = tiles // 2
    first = lax.axis_index("tiles") * tiles
    odd = lax.axis_index("tiles") % 2
    for side, bits in ((1 - odd, inner_bits), (odd, outer_bits)):
        together = outs.pop(0)
        alone = {n: outs.pop(0) for n in bits}
        for i in range(half):
            row = tiles_ref[first + side * half + i] - first
            for n in range(near):
                tile = pieces[n][row]
                together[n, i] = tile
                if n in alone:
                    alone[n][i] = tile


def split(group):
    near = [0] + [1 << n for n in range(group.bit_length() - 1)]
    return near, [m for m in range(group) if m not in near]


def tile_of(group, side, tile):
    near, far = split(group)
    cut = {m: side[0][n, tile] for n, m in enumerate(near)} | {m: side[1 + n][tile] for n, m in enumerate(far)}
    return jnp.concatenate([cut[m] for m in range(group)], axis=0)


def assemble_kernel(group, perm_ref, *refs):
    *pieces, tiles_ref, weight_ref = refs
    perm = perm_ref[...]
    odd = lax.axis_index("tiles") % 2
    per_side = (len(pieces) - group) // 2

    def step(base, side, i, carry):
        pair = [tile_of(group, side, 2 * i + j) for j in range(2)]
        got = jnp.dot(perm, jnp.concatenate(pair, axis=1), preferred_element_type=jnp.float32)
        for j in range(2):
            tiles_ref[base + 2 * i + j] = got[:, j * LANES : (j + 1) * LANES].astype(jnp.bfloat16)
        return carry

    for n in range(2):
        side = pieces[n * per_side : (n + 1) * per_side]
        half = side[0].shape[1]
        base = jnp.where(odd == n, 2 * half, half)
        lax.fori_loop(0, half // 2, functools.partial(step, base, side), 0, unroll=4)
    weights = pieces[2 * per_side :]
    me = lax.axis_index("feat")
    features = weights[0].shape[1]
    rows = []
    for rank in range(group):
        row = weights[0][...].astype(jnp.float32)
        for m in range(1, group):
            row = jnp.where(me ^ m == rank, weights[m][...].astype(jnp.float32), row)
        rows.append(row)
    weight_ref[...] = jnp.zeros_like(weight_ref)
    weight_ref[:features, :features] = jnp.concatenate(rows, axis=0).astype(jnp.bfloat16)


def mask_accumulators(dst, per_row):
    shape = (2 * dst, 2 * LANES)
    return [[[pltpu.ACC(q)(shape, jnp.float32) for _ in range(per_row // 2)] for _ in range(2)] for q in range(2)]


def emptied(accs):
    for a in accs:
        pltpu.matmul_pop(a)


def sum_rows(group, dst, per_row, start, accs, neighbours_ref, held, chunk_refs, sums_ref, degrees_ref):
    emptied([a for by_mxu in accs for by_set in by_mxu for a in by_set])
    me = lax.axis_index("feat")
    slots, words = chunk_refs[0][0].shape[1:3]
    tiles, half = neighbours_ref.shape[1], held.shape[0] // 4
    features = held.shape[2]
    origin = lax.axis_index("tiles") * tiles - half
    pairs = per_row // 2
    one, zero = jnp.bfloat16(1), jnp.bfloat16(0)
    upper = lax.broadcasted_iota(jnp.int32, (2 * SUB, LANES), 0) >= SUB
    bits = [jnp.where(upper, 2 << b, 1 << b).astype(jnp.int16) for b in range(0, BITS - 1, 2)]

    def source(slot, tile):
        return jnp.clip(neighbours_ref[slot, tile] - origin, 0, 4 * half - 1)

    def finished(which):
        got = [pltpu.matmul_pop(accs[0][which][p]) + pltpu.matmul_pop(accs[1][which][p]) for p in range(pairs)]
        return jnp.concatenate(
            [s[j * dst : (j + 1) * dst, j * features : (j + 1) * features] for s in got for j in range(2)], axis=0
        )

    def row_of(words_refs, first, row, which):
        tile = (start + row) * per_row
        count = jnp.zeros((SUB, LANES), jnp.int32)
        turn = 0
        for m in range(group):
            for k in range(slots):
                slot = (me ^ m) * slots + k
                parts = [words_refs[m][row - first, k, w : w + SUB] for w in range(0, words, SUB)]
                for part in parts:
                    count = count + lax.population_count(part.astype(jnp.int32))
                front = jnp.concatenate(parts[:-1], axis=0)
                back = jnp.concatenate([parts[-1]] * 2, axis=0)
                planes = [jnp.where((front & jnp.int16(1 << b)) != 0, one, zero) for b in range(BITS)]
                planes += [jnp.where((back & bit) != 0, one, zero) for bit in bits]
                mask = jnp.concatenate(planes, axis=0).T
                mxu = turn % 2
                for p in range(pairs):
                    s0, s1 = (source(slot, tile + 2 * p + j) for j in range(2))
                    register = (turn // 2 * pairs + p) % 2
                    pltpu.matmul_push_rhs(jnp.concatenate([held[s0], held[s1]], axis=1), register, mxu)
                    part = mask[2 * p * dst : 2 * (p + 1) * dst]
                    pltpu.matmul_acc_lhs(accs[mxu][which][p], part, load_staged_rhs=register)
                turn += 1
                if turn == 6:
                    sums_ref[row] = finished(1 - which)
        degrees_ref[row] = jnp.broadcast_to(jnp.sum(count, axis=0, keepdims=True), (SUB, LANES)).astype(jnp.float32)

    first = 0
    for words_refs in chunk_refs:
        size = words_refs[0].shape[0]
        count = 4 if size % 4 == 0 else 2

        def step(n, carry, words_refs=words_refs, first=first, count=count):
            for j in range(count):
                row_of(words_refs, first, first + count * n + j, j % 2)
            return carry

        lax.fori_loop(0, size // count, step, 0)
        first += size
    sums_ref[first] = finished(1)


def early_kernel(group, dst, per_row, neighbours_ref, perm_ref, *refs):
    whole = [[pltpu.ACC(q)((2 * LANES, 2 * LANES), jnp.float32) for _ in range(2)] for q in range(2)]

    def body(accs, whole):
        _, far = split(group)
        per_side = 1 + len(far)
        sides = [refs[n * per_side : (n + 1) * per_side] for n in range(2)]
        held, sums_ref, degrees_ref = refs[-3:]
        words = refs[2 * per_side : -4]
        half = sides[0][0].shape[1]
        odd = lax.axis_index("tiles") % 2
        bases = [jnp.where(odd == q, 3 * half, 0) for q in range(2)]
        emptied(whole[0] + whole[1])
        perm = perm_ref[...]

        def step(i, carry):
            for n in range(2):
                for q in range(2):
                    pair = [tile_of(group, sides[q], 4 * i + 2 * n + j) for j in range(2)]
                    pltpu.matmul_push_rhs(jnp.concatenate(pair, axis=1), n, q)
                    pltpu.matmul_acc_lhs(whole[q][n], perm, load_staged_rhs=n)
            for n in range(2):
                for q in range(2):
                    got = pltpu.matmul_pop(whole[q][n])
                    for j in range(2):
                        tile = got[:, j * LANES : (j + 1) * LANES]
                        held[bases[q] + 4 * i + 2 * n + j] = tile.astype(jnp.bfloat16)
            return carry

        lax.fori_loop(0, half // 4, step, 0, unroll=2)
        chunk_refs = [words[n : n + group] for n in range(0, len(words), group)]
        sum_rows(group, dst, per_row, 0, accs, neighbours_ref, held, chunk_refs, sums_ref, degrees_ref)

    pl.run_scoped(body, mask_accumulators(dst, per_row), whole)


def late_kernel(group, dst, per_row, neighbours_ref, *refs):
    def body(accs, products):
        held, weight_ref, bias_ref, feats_ref, *words, early_sums, early_degrees = refs[:-5]
        out_ref, sums_ref, degrees_ref, result_ref, sem = refs[-5:]
        emptied(products)
        features = bias_ref.shape[1]
        bias = bias_ref[...]
        start = early_degrees.shape[0]

        def finish(start, sums_ref, degrees_ref, turn):
            rows = degrees_ref.shape[0]
            for n in range(0, rows, 2):
                bases, wide = [], []
                for row in range(n, n + 2):
                    scale = jnp.sqrt(degrees_ref[row] + 1.0).T[:, :1]
                    own = feats_ref[(start + row) * per_row : (start + row + 1) * per_row]
                    base = own.reshape(LANES, features).astype(jnp.float32)
                    normed = ((sums_ref[row + 1] + base) / scale).astype(jnp.bfloat16)
                    bases.append(base)
                    wide.append(jnp.concatenate([normed, jnp.zeros_like(normed)], axis=1))
                q = n // 2 % 2
                if n < 4:
                    pltpu.matmul_push_rhs(weight_ref[...], 0, q)
                lhs = jnp.concatenate(wide, axis=0)
                pltpu.matmul_acc_lhs(products[q], lhs, load_staged_rhs=0 if n < 4 else None)
                linear = pltpu.matmul_pop(products[q])[:, :features] + bias
                result = (jnp.concatenate(bases, axis=0) + jnp.maximum(linear, 0.0)).astype(jnp.bfloat16)
                at = (start + n) * per_row
                result_ref[at : at + 2 * per_row] = result.reshape(2 * per_row, dst, features)
            part = pl.ds(start * per_row, rows * per_row)
            return pltpu.make_async_copy(result_ref.at[part], out_ref.at[part], sem.at[turn])

        first = finish(0, early_sums, early_degrees, 0)
        first.start()
        sum_rows(group, dst, per_row, start, accs, neighbours_ref, held, [words], sums_ref, degrees_ref)
        last = finish(start, sums_ref, degrees_ref, 1)
        last.start()
        first.wait()
        last.wait()

    products = [pltpu.ACC(q)((2 * LANES, 2 * LANES), jnp.float32) for q in range(2)]
    pl.run_scoped(body, mask_accumulators(dst, per_row), products)


def swap(x, group, m):
    return lax.ppermute(x, "feat", [(i, i ^ m) for i in range(group)])


def per_device(feats, weight, bias, neighbours, counts, adj_words, tile_row):
    group, bands = lax.axis_size("feat"), lax.axis_size("tiles")
    me = lax.axis_index("feat")
    tiles, dst, features = feats.shape
    _, slots, words, cells = adj_words.shape
    half = tiles // 2
    per_row = LANES // dst
    rows = tiles // per_row
    assert half >= REACH and rows % 4 == 0 and per_row % 2 == 0 and bands % 2 == 0 and features == LANES
    sizes = [rows // 4, rows // 4, rows // 2] if rows % 8 == 0 else [rows // 2, rows // 2]

    shapes = [jax.ShapeDtypeStruct((n, slots, words, LANES), jnp.int16) for n in sizes for _ in range(group)]
    block = math.gcd(*sizes) * per_row
    packed = pl.pallas_call(
        lambda *refs: pack_kernel(group, dst, per_row, BITS - (words * BITS - cells), sizes, *refs),
        out_shape=shapes,
        grid=(tiles // block,),
        in_specs=[SMEM, pl.BlockSpec((block, slots, words, cells), lambda i: (i, 0, 0, 0))],
        out_specs=[pl.BlockSpec(s.shape, lambda i: (0, 0, 0, 0)) for s in shapes],
        cost_estimate=pl.CostEstimate(flops=3 * 10**9, bytes_accessed=5 * 10**6, transcendentals=0),
        name="pack",
    )(counts, adj_words)

    direct = [1 << n for n in range(group.bit_length() - 1)]
    far = [m for m in range(group) if m & (m - 1)]
    near = [feats] + [swap(feats, group, m) for m in direct]
    weight_pieces = [weight] + [swap(weight, group, m) for m in range(1, group)]
    inner_bits = list(range(1, len(direct)))
    outer_bits = list(range(2, len(direct) + 1))
    together = jax.ShapeDtypeStruct((len(near), half, dst, features), jnp.bfloat16)
    alone = jax.ShapeDtypeStruct((half, dst, features), jnp.bfloat16)
    inner, *rest = pl.pallas_call(
        lambda *refs: arrange_kernel(len(near), inner_bits, outer_bits, *refs),
        out_shape=[together] + [alone] * len(inner_bits) + [together] + [alone] * len(outer_bits),
        in_specs=[SMEM] + [VMEM] * len(near),
        out_specs=[VMEM] * (2 + len(inner_bits) + len(outer_bits)),
        compiler_params=pltpu.CompilerParams(vmem_limit_bytes=4 * 2**20),
        cost_estimate=pl.CostEstimate(flops=10**9, bytes_accessed=10**6, transcendentals=0),
        name="arrange",
    )(tile_row, *near)
    inners = {direct[n - 1]: part for n, part in zip(inner_bits, rest)}
    outer, *rest = rest[len(inner_bits) :]
    outers = {direct[n - 1]: part for n, part in zip(outer_bits, rest)}
    for m in far:
        bits = [bit for bit in direct if m & bit]
        inners[m] = swap(inners[m ^ bits[-1]], group, bits[-1])
        outers[m] = swap(outers[m ^ bits[0]], group, bits[0])
    inners, outers = [inner] + [inners[m] for m in far], [outer] + [outers[m] for m in far]
    exchanged = []
    for c in range(len(sizes)):
        parts = packed[c * group : (c + 1) * group]
        exchanged += [parts[0]] + [swap(parts[m], group, m) for m in range(1, group)]

    inside = [(i, i ^ 1) for i in range(bands)]
    across = [pair for i in range(1, bands - 1, 2) for pair in ((i, i + 1), (i + 1, i))]
    from_inside, from_across = [], []
    for n in range(len(inners)):
        from_across.append(lax.ppermute(outers[n], "tiles", across))
        from_inside.append(lax.ppermute(inners[n], "tiles", inside))

    cell = row_cells(words, cells)
    column = ((cell // dst) ^ me) * dst + cell % dst
    perm = (column[:, None] == jnp.arange(cells, dtype=jnp.int32)[None, :]).astype(jnp.bfloat16)
    reachable = jax.ShapeDtypeStruct((4 * half, cells, features), jnp.bfloat16)
    sides = inners + outers + weight_pieces
    own_tiles, weight_wide = pl.pallas_call(
        lambda *refs: assemble_kernel(group, *refs),
        out_shape=[reachable, jax.ShapeDtypeStruct((2 * features, 2 * features), jnp.bfloat16)],
        in_specs=[VMEM] * (1 + len(sides)),
        out_specs=[VMEM] * 2,
        compiler_params=pltpu.CompilerParams(vmem_limit_bytes=4 * 2**20),
        cost_estimate=pl.CostEstimate(flops=2 * 10**9, bytes_accessed=4 * 10**6, transcendentals=0),
        name="assemble",
    )(perm, *sides)

    late = sizes[-1]
    early = rows - late
    sides = from_inside + from_across
    parts = exchanged[:-group]
    all_tiles, early_sums, early_degrees = pl.pallas_call(
        lambda *refs: early_kernel(group, dst, per_row, *refs),
        out_shape=[
            reachable,
            jax.ShapeDtypeStruct((early + 1, LANES, features), jnp.float32),
            jax.ShapeDtypeStruct((early, SUB, LANES), jnp.float32),
        ],
        in_specs=[SMEM] + [VMEM] * (2 + len(sides) + len(parts)),
        out_specs=[VMEM] * 3,
        input_output_aliases={2 + len(sides) + len(parts): 0},
        compiler_params=pltpu.CompilerParams(vmem_limit_bytes=12 * 2**20),
        cost_estimate=pl.CostEstimate(flops=10**10, bytes_accessed=10**7, transcendentals=0),
        name="early",
    )(neighbours.T, perm, *sides, *parts, own_tiles)
    parts = exchanged[-group:]
    return pl.pallas_call(
        lambda *refs: late_kernel(group, dst, per_row, *refs),
        out_shape=jax.ShapeDtypeStruct(feats.shape, feats.dtype),
        in_specs=[SMEM] + [VMEM] * (6 + len(parts)),
        out_specs=HBM,
        scratch_shapes=[
            pltpu.VMEM((late + 1, LANES, features), jnp.float32),
            pltpu.VMEM((late, SUB, LANES), jnp.float32),
            pltpu.VMEM(feats.shape, jnp.bfloat16),
            pltpu.SemaphoreType.DMA((2,)),
        ],
        compiler_params=pltpu.CompilerParams(vmem_limit_bytes=12 * 2**20),
        cost_estimate=pl.CostEstimate(flops=10**10, bytes_accessed=10**7, transcendentals=0),
        name="late",
    )(neighbours.T, all_tiles, weight_wide, bias[None, :], feats, *parts, early_sums, early_degrees)


def solution(mesh):
    return jax.shard_map(
        per_device,
        mesh=mesh,
        in_specs=(
            P("tiles", "feat", None),
            P("feat", None),
            P(),
            P("tiles", None),
            P("tiles"),
            P("tiles", "feat", None, None),
            P(),
        ),
        out_specs=P("tiles", "feat", None),
        check_vma=False,
    )
```

```python
import functools
import math

import jax
import jax.numpy as jnp
import numpy as np
from jax import lax
from jax.experimental import pallas as pl
from jax.experimental.pallas import tpu as pltpu
from jax.sharding import PartitionSpec as P

BITS = 11
LANES = 128
SUB = 8
REACH = 16


HBM = pl.BlockSpec(memory_space=pltpu.HBM)
SMEM = pl.BlockSpec(memory_space=pltpu.SMEM)
VMEM = pl.BlockSpec(memory_space=pltpu.VMEM)


def row_cells(words, cells):
    spare = words * BITS - cells
    assert spare == SUB and words % SUB == 0
    last, tail = BITS - spare, words - SUB
    order = [(b, w) for b in range(BITS) for w in range(tail)]
    order += [(b, w) for b in range(BITS - 1) for w in range(tail, words)]
    out = []
    for b, w in order:
        moved = w == words - 1 and b >= last
        out.append((tail + b - last) * BITS + BITS - 1 if moved else w * BITS + b)
    assert sorted(out) == list(range(cells))
    return np.array(out, dtype=np.int32)


def pack_kernel(group, dst, per_row, last, sizes, counts_ref, words_ref, *out_refs):
    me = lax.axis_index("feat")
    tiles, slots, words, cells = words_ref.shape
    rows = tiles // per_row
    lane = lax.broadcasted_iota(jnp.int32, (words, LANES), 1)
    sub = lax.broadcasted_iota(jnp.int32, (SUB, cells), 0)

    def row_of(rank, at, c, g, carry):
        for k in range(slots):
            packed = []
            for i in range(per_row):
                tile = g * per_row + i
                live = rank * slots + k < counts_ref[pl.program_id(0) * tiles + tile]
                both = jnp.where(live, words_ref[tile, k], 0)
                tail = both[words - SUB :]
                top = ((tail >> (BITS - 1)) & 1) << (sub + last)
                moved = jnp.sum(top, axis=0, keepdims=True)
                kept = tail & ((1 << (BITS - 1)) - 1)
                tail = jnp.where(sub == SUB - 1, kept | moved, kept)
                packed.append(jnp.concatenate([both[: words - SUB], tail], axis=0))
            for m in range(group):
                start = (rank ^ m) * dst
                block, offset = start // LANES, start % LANES
                row = None
                for i in range(per_row):
                    piece = packed[i][:, block * LANES : (block + 1) * LANES]
                    shift = (i * dst + LANES - offset) % LANES
                    if shift:
                        piece = pltpu.roll(piece, shift, 1)
                    row = piece if row is None else jnp.where(lane >= i * dst, piece, row)
                out_refs[c * group + m][at + g, k] = row.astype(jnp.int16)
        return carry

    for rank in range(group):
        at = 0
        for c, size in enumerate(sizes):
            first, step = at // rows, pl.program_id(0)

            @pl.when((me == rank) & (step >= first) & (step < first + size // rows))
            def _(rank=rank, c=c, first=first):
                lax.fori_loop(0, rows, functools.partial(row_of, rank, (step - first) * rows, c), 0, unroll=max(1, min(rows, 16 // group)))

            at += size


def arrange_kernel(near, inner_bits, outer_bits, tiles_ref, *refs):
    pieces, outs = refs[:near], list(refs[near:])
    tiles = pieces[0].shape[0]
    half = tiles // 2
    first = lax.axis_index("tiles") * tiles
    odd = lax.axis_index("tiles") % 2
    for side, bits in ((1 - odd, inner_bits), (odd, outer_bits)):
        together = outs.pop(0)
        alone = {n: outs.pop(0) for n in bits}
        for i in range(half):
            row = tiles_ref[first + side * half + i] - first
            for n in range(near):
                tile = pieces[n][row]
                together[n, i] = tile
                if n in alone:
                    alone[n][i] = tile


def split(group):
    near = [0] + [1 << n for n in range(group.bit_length() - 1)]
    return near, [m for m in range(group) if m not in near]


def tile_of(group, side, tile):
    near, far = split(group)
    cut = {m: side[0][n, tile] for n, m in enumerate(near)} | {m: side[1 + n][tile] for n, m in enumerate(far)}
    return jnp.concatenate([cut[m] for m in range(group)], axis=0)


def assemble_kernel(group, perm_ref, *refs):
    *pieces, tiles_ref, weight_ref = refs
    perm = perm_ref[...]
    odd = lax.axis_index("tiles") % 2
    per_side = (len(pieces) - group) // 2

    def step(base, side, i, carry):
        pair = [tile_of(group, side, 2 * i + j) for j in range(2)]
        got = jnp.dot(perm, jnp.concatenate(pair, axis=1), preferred_element_type=jnp.float32)
        for j in range(2):
            tiles_ref[base + 2 * i + j] = got[:, j * LANES : (j + 1) * LANES].astype(jnp.bfloat16)
        return carry

    for n in range(2):
        side = pieces[n * per_side : (n + 1) * per_side]
        half = side[0].shape[1]
        base = jnp.where(odd == n, 2 * half, half)
        lax.fori_loop(0, half // 2, functools.partial(step, base, side), 0, unroll=4)
    weights = pieces[2 * per_side :]
    me = lax.axis_index("feat")
    features = weights[0].shape[1]
    rows = []
    for rank in range(group):
        row = weights[0][...].astype(jnp.float32)
        for m in range(1, group):
            row = jnp.where(me ^ m == rank, weights[m][...].astype(jnp.float32), row)
        rows.append(row)
    weight_ref[...] = jnp.zeros_like(weight_ref)
    weight_ref[:features, :features] = jnp.concatenate(rows, axis=0).astype(jnp.bfloat16)


def mask_accumulators(dst, per_row):
    shape = (2 * dst, 2 * LANES)
    return [[[pltpu.ACC(q)(shape, jnp.float32) for _ in range(per_row // 2)] for _ in range(2)] for q in range(2)]


def emptied(accs):
    for a in accs:
        pltpu.matmul_pop(a)


def sum_rows(group, dst, per_row, start, accs, neighbours_ref, held, chunk_refs, sums_ref, degrees_ref):
    emptied([a for by_mxu in accs for by_set in by_mxu for a in by_set])
    me = lax.axis_index("feat")
    slots, words = chunk_refs[0][0].shape[1:3]
    tiles, half = neighbours_ref.shape[1], held.shape[0] // 4
    features = held.shape[2]
    origin = lax.axis_index("tiles") * tiles - half
    pairs = per_row // 2
    one, zero = jnp.bfloat16(1), jnp.bfloat16(0)
    upper = lax.broadcasted_iota(jnp.int32, (2 * SUB, LANES), 0) >= SUB
    bits = [jnp.where(upper, 2 << b, 1 << b).astype(jnp.int16) for b in range(0, BITS - 1, 2)]

    def source(slot, tile):
        return jnp.clip(neighbours_ref[slot, tile] - origin, 0, 4 * half - 1)

    def finished(which):
        got = [pltpu.matmul_pop(accs[0][which][p]) + pltpu.matmul_pop(accs[1][which][p]) for p in range(pairs)]
        return jnp.concatenate(
            [s[j * dst : (j + 1) * dst, j * features : (j + 1) * features] for s in got for j in range(2)], axis=0
        )

    def row_of(words_refs, first, row, which):
        tile = (start + row) * per_row
        count = jnp.zeros((SUB, LANES), jnp.int32)
        turn = 0
        for m in range(group):
            for k in range(slots):
                slot = (me ^ m) * slots + k
                parts = [words_refs[m][row - first, k, w : w + SUB] for w in range(0, words, SUB)]
                for part in parts:
                    count = count + lax.population_count(part.astype(jnp.int32))
                front = jnp.concatenate(parts[:-1], axis=0)
                back = jnp.concatenate([parts[-1]] * 2, axis=0)
                planes = [jnp.where((front & jnp.int16(1 << b)) != 0, one, zero) for b in range(BITS)]
                planes += [jnp.where((back & bit) != 0, one, zero) for bit in bits]
                mask = jnp.concatenate(planes, axis=0).T
                mxu = turn % 2
                for p in range(pairs):
                    s0, s1 = (source(slot, tile + 2 * p + j) for j in range(2))
                    register = (turn // 2 * pairs + p) % 2
                    pltpu.matmul_push_rhs(jnp.concatenate([held[s0], held[s1]], axis=1), register, mxu)
                    part = mask[2 * p * dst : 2 * (p + 1) * dst]
                    pltpu.matmul_acc_lhs(accs[mxu][which][p], part, load_staged_rhs=register)
                turn += 1
                if turn == 6:
                    sums_ref[row] = finished(1 - which)
        degrees_ref[row] = jnp.broadcast_to(jnp.sum(count, axis=0, keepdims=True), (SUB, LANES)).astype(jnp.float32)

    first = 0
    for words_refs in chunk_refs:
        size = words_refs[0].shape[0]
        count = 4 if size % 4 == 0 else 2

        def step(n, carry, words_refs=words_refs, first=first, count=count):
            for j in range(count):
                row_of(words_refs, first, first + count * n + j, j % 2)
            return carry

        lax.fori_loop(0, size // count, step, 0)
        first += size
    sums_ref[first] = finished(1)


def early_kernel(group, dst, per_row, table_ref, perm_ref, *refs):
    whole = [[pltpu.ACC(q)((2 * LANES, 2 * LANES), jnp.float32) for _ in range(2)] for q in range(2)]

    def body(accs, whole):
        _, far = split(group)
        per_side = 1 + len(far)
        sides = [refs[n * per_side : (n + 1) * per_side] for n in range(2)]
        held, sums_ref, degrees_ref, neighbours_ref, sem = refs[-5:]
        words = refs[2 * per_side : -6]
        table = pltpu.make_async_copy(table_ref, neighbours_ref, sem)
        table.start()
        half = sides[0][0].shape[1]
        odd = lax.axis_index("tiles") % 2
        bases = [jnp.where(odd == q, 3 * half, 0) for q in range(2)]
        emptied(whole[0] + whole[1])
        perm = perm_ref[...]

        def step(i, carry):
            for n in range(2):
                for q in range(2):
                    pair = [tile_of(group, sides[q], 4 * i + 2 * n + j) for j in range(2)]
                    pltpu.matmul_push_rhs(jnp.concatenate(pair, axis=1), n, q)
                    pltpu.matmul_acc_lhs(whole[q][n], perm, load_staged_rhs=n)
            for n in range(2):
                for q in range(2):
                    got = pltpu.matmul_pop(whole[q][n])
                    for j in range(2):
                        tile = got[:, j * LANES : (j + 1) * LANES]
                        held[bases[q] + 4 * i + 2 * n + j] = tile.astype(jnp.bfloat16)
            return carry

        lax.fori_loop(0, half // 4, step, 0, unroll=2)
        table.wait()
        chunk_refs = [words[n : n + group] for n in range(0, len(words), group)]
        sum_rows(group, dst, per_row, 0, accs, neighbours_ref, held, chunk_refs, sums_ref, degrees_ref)

    pl.run_scoped(body, mask_accumulators(dst, per_row), whole)


def late_kernel(group, dst, per_row, table_ref, *refs):
    def body(accs, products):
        held, weight_ref, bias_ref, feats_ref, *words, early_sums, early_degrees = refs[:-6]
        out_ref, sums_ref, degrees_ref, result_ref, neighbours_ref, sem = refs[-6:]
        table = pltpu.make_async_copy(table_ref, neighbours_ref, sem.at[2])
        table.start()
        emptied(products)
        features = bias_ref.shape[1]
        bias = bias_ref[...]
        start = early_degrees.shape[0]

        def finish(start, sums_ref, degrees_ref, turn):
            rows = degrees_ref.shape[0]
            for n in range(0, rows, 2):
                bases, wide = [], []
                for row in range(n, n + 2):
                    scale = (1.0 / jnp.sqrt(degrees_ref[row] + 1.0)).T[:, :1]
                    own = feats_ref[(start + row) * per_row : (start + row + 1) * per_row]
                    base = own.reshape(LANES, features).astype(jnp.float32)
                    normed = ((sums_ref[row + 1] + base) * scale).astype(jnp.bfloat16)
                    bases.append(base)
                    wide.append(jnp.concatenate([normed, jnp.zeros_like(normed)], axis=1))
                q = n // 2 % 2
                if n < 4:
                    pltpu.matmul_push_rhs(weight_ref[...], 0, q)
                lhs = jnp.concatenate(wide, axis=0)
                pltpu.matmul_acc_lhs(products[q], lhs, load_staged_rhs=0 if n < 4 else None)
                linear = pltpu.matmul_pop(products[q])[:, :features] + bias
                result = (jnp.concatenate(bases, axis=0) + jnp.maximum(linear, 0.0)).astype(jnp.bfloat16)
                at = (start + n) * per_row
                result_ref[at : at + 2 * per_row] = result.reshape(2 * per_row, dst, features)
            part = pl.ds(start * per_row, rows * per_row)
            return pltpu.make_async_copy(result_ref.at[part], out_ref.at[part], sem.at[turn])

        first = finish(0, early_sums, early_degrees, 0)
        first.start()
        table.wait()
        sum_rows(group, dst, per_row, start, accs, neighbours_ref, held, [words], sums_ref, degrees_ref)
        last = finish(start, sums_ref, degrees_ref, 1)
        last.start()
        first.wait()
        last.wait()

    products = [pltpu.ACC(q)((2 * LANES, 2 * LANES), jnp.float32) for q in range(2)]
    pl.run_scoped(body, mask_accumulators(dst, per_row), products)


def swap(x, group, m):
    return lax.ppermute(x, "feat", [(i, i ^ m) for i in range(group)])


def per_device(feats, weight, bias, neighbours, counts, adj_words, tile_row):
    group, bands = lax.axis_size("feat"), lax.axis_size("tiles")
    me = lax.axis_index("feat")
    tiles, dst, features = feats.shape
    _, slots, words, cells = adj_words.shape
    half = tiles // 2
    per_row = LANES // dst
    rows = tiles // per_row
    assert half >= REACH and rows % 4 == 0 and per_row % 2 == 0 and bands % 2 == 0 and features == LANES
    sizes = [rows // 4, rows // 4, rows // 2] if rows % 8 == 0 else [rows // 2, rows // 2]

    shapes = [jax.ShapeDtypeStruct((n, slots, words, LANES), jnp.int16) for n in sizes for _ in range(group)]
    block = math.gcd(*sizes) * per_row
    packed = pl.pallas_call(
        lambda *refs: pack_kernel(group, dst, per_row, BITS - (words * BITS - cells), sizes, *refs),
        out_shape=shapes,
        grid=(tiles // block,),
        in_specs=[SMEM, pl.BlockSpec((block, slots, words, cells), lambda i: (i, 0, 0, 0))],
        out_specs=[pl.BlockSpec(s.shape, lambda i: (0, 0, 0, 0)) for s in shapes],
        cost_estimate=pl.CostEstimate(flops=3 * 10**9, bytes_accessed=5 * 10**6, transcendentals=0),
        name="pack",
    )(counts, adj_words)

    direct = [1 << n for n in range(group.bit_length() - 1)]
    far = [m for m in range(group) if m & (m - 1)]
    near = [feats] + [swap(feats, group, m) for m in direct]
    weight_pieces = [weight] + [swap(weight, group, m) for m in range(1, group)]
    inner_bits = list(range(1, len(direct)))
    outer_bits = list(range(2, len(direct) + 1))
    together = jax.ShapeDtypeStruct((len(near), half, dst, features), jnp.bfloat16)
    alone = jax.ShapeDtypeStruct((half, dst, features), jnp.bfloat16)
    inner, *rest = pl.pallas_call(
        lambda *refs: arrange_kernel(len(near), inner_bits, outer_bits, *refs),
        out_shape=[together] + [alone] * len(inner_bits) + [together] + [alone] * len(outer_bits),
        in_specs=[SMEM] + [VMEM] * len(near),
        out_specs=[VMEM] * (2 + len(inner_bits) + len(outer_bits)),
        compiler_params=pltpu.CompilerParams(vmem_limit_bytes=4 * 2**20),
        cost_estimate=pl.CostEstimate(flops=10**9, bytes_accessed=10**6, transcendentals=0),
        name="arrange",
    )(tile_row, *near)
    inners = {direct[n - 1]: part for n, part in zip(inner_bits, rest)}
    outer, *rest = rest[len(inner_bits) :]
    outers = {direct[n - 1]: part for n, part in zip(outer_bits, rest)}
    for m in far:
        bits = [bit for bit in direct if m & bit]
        inners[m] = swap(inners[m ^ bits[-1]], group, bits[-1])
        outers[m] = swap(outers[m ^ bits[0]], group, bits[0])
    inners, outers = [inner] + [inners[m] for m in far], [outer] + [outers[m] for m in far]
    exchanged = []
    for c in range(len(sizes)):
        parts = packed[c * group : (c + 1) * group]
        exchanged += [parts[0]] + [swap(parts[m], group, m) for m in range(1, group)]

    inside = [(i, i ^ 1) for i in range(bands)]
    across = [pair for i in range(1, bands - 1, 2) for pair in ((i, i + 1), (i + 1, i))]
    from_inside, from_across = [], []
    for n in range(len(inners)):
        from_across.append(lax.ppermute(outers[n], "tiles", across))
        from_inside.append(lax.ppermute(inners[n], "tiles", inside))

    cell = row_cells(words, cells)
    column = ((cell // dst) ^ me) * dst + cell % dst
    perm = (column[:, None] == jnp.arange(cells, dtype=jnp.int32)[None, :]).astype(jnp.bfloat16)
    reachable = jax.ShapeDtypeStruct((4 * half, cells, features), jnp.bfloat16)
    sides = inners + outers + weight_pieces
    own_tiles, weight_wide = pl.pallas_call(
        lambda *refs: assemble_kernel(group, *refs),
        out_shape=[reachable, jax.ShapeDtypeStruct((2 * features, 2 * features), jnp.bfloat16)],
        in_specs=[VMEM] * (1 + len(sides)),
        out_specs=[VMEM] * 2,
        compiler_params=pltpu.CompilerParams(vmem_limit_bytes=4 * 2**20),
        cost_estimate=pl.CostEstimate(flops=2 * 10**9, bytes_accessed=4 * 10**6, transcendentals=0),
        name="assemble",
    )(perm, *sides)

    late = sizes[-1]
    early = rows - late
    sides = from_inside + from_across
    parts = exchanged[:-group]
    all_tiles, early_sums, early_degrees = pl.pallas_call(
        lambda *refs: early_kernel(group, dst, per_row, *refs),
        out_shape=[
            reachable,
            jax.ShapeDtypeStruct((early + 1, LANES, features), jnp.float32),
            jax.ShapeDtypeStruct((early, SUB, LANES), jnp.float32),
        ],
        in_specs=[VMEM] * (3 + len(sides) + len(parts)),
        out_specs=[VMEM] * 3,
        scratch_shapes=[pltpu.SMEM(neighbours.shape[::-1], jnp.int32), pltpu.SemaphoreType.DMA],
        input_output_aliases={2 + len(sides) + len(parts): 0},
        compiler_params=pltpu.CompilerParams(vmem_limit_bytes=12 * 2**20),
        cost_estimate=pl.CostEstimate(flops=10**10, bytes_accessed=10**7, transcendentals=0),
        name="early",
    )(neighbours.T, perm, *sides, *parts, own_tiles)
    parts = exchanged[-group:]
    return pl.pallas_call(
        lambda *refs: late_kernel(group, dst, per_row, *refs),
        out_shape=jax.ShapeDtypeStruct(feats.shape, feats.dtype),
        in_specs=[VMEM] * (7 + len(parts)),
        out_specs=HBM,
        scratch_shapes=[
            pltpu.VMEM((late + 1, LANES, features), jnp.float32),
            pltpu.VMEM((late, SUB, LANES), jnp.float32),
            pltpu.VMEM(feats.shape, jnp.bfloat16),
            pltpu.SMEM(neighbours.shape[::-1], jnp.int32),
            pltpu.SemaphoreType.DMA((3,)),
        ],
        compiler_params=pltpu.CompilerParams(vmem_limit_bytes=12 * 2**20),
        cost_estimate=pl.CostEstimate(flops=10**10, bytes_accessed=10**7, transcendentals=0),
        name="late",
    )(neighbours.T, all_tiles, weight_wide, bias[None, :], feats, *parts, early_sums, early_degrees)


def solution(mesh):
    return jax.shard_map(
        per_device,
        mesh=mesh,
        in_specs=(
            P("tiles", "feat", None),
            P("feat", None),
            P(),
            P("tiles", None),
            P("tiles"),
            P("tiles", "feat", None, None),
            P(),
        ),
        out_specs=P("tiles", "feat", None),
        check_vma=False,
    )
```
